8 devices in a mesh: b: 1 (over z), rep: 2 (over y), col: 2 (over x), row: 2 (over core).
Axes of the slice: x: 2, y: 2, z: 1, core: 2. Of those that a mesh axis runs over, the one named last changes fastest.
Arguments:
- a_blocks: float32 [64, 64, 128, 128], P(('b', 'row'), 'col')
Outputs:
- output: float32 [64, 64, 128, 128], P(('b', 'row'), 'col')
All inputs are finite; a program needn't handle non-finite values.
Results may differ from the reference program's by a relative error of at most 0.001.
Values sent between devices are 32-bit elements.
A program may use at most 1 GiB of HBM per device.

```python
import jax
import jax.numpy as jnp
from jax import lax

N = 8192
NB = 128
ROW = 2
COL = 2
RANK = N // 8
NUM_BLK = N // NB
ROW_BLK = NUM_BLK // ROW
COL_BLK = NUM_BLK // COL


def to_cyclic(natural):
    grid_view = natural.reshape(ROW_BLK, ROW, NB, COL_BLK, COL, NB)
    return grid_view.transpose(1, 0, 4, 3, 2, 5).reshape(NUM_BLK, NUM_BLK, NB, NB)


def from_cyclic(blocks):
    grid_view = blocks.reshape(ROW, ROW_BLK, COL, COL_BLK, NB, NB)
    return grid_view.transpose(1, 0, 4, 3, 2, 5).reshape(N, N)


def setup_inputs(seed: int = 0, part: int = 0) -> dict:
    base_key = jax.random.fold_in(jax.random.key(seed), part)
    factor = jax.random.normal(base_key, (N, RANK), jnp.float32)
    gram_mat = jnp.dot(factor, factor.T, precision=lax.Precision.HIGHEST, preferred_element_type=jnp.float32)
    spd_mat = 0.5 * (gram_mat + gram_mat.T) + RANK * jnp.eye(N, dtype=jnp.float32)
    return {"a_blocks": to_cyclic(spd_mat)}


def reference(a_blocks):
    lower_fac = jnp.tril(jnp.linalg.cholesky(from_cyclic(a_blocks)))
    return to_cyclic(lower_fac)
```

```python
import jax
import jax.numpy as jnp
from jax import lax
from jax.experimental import pallas as pl
from jax.experimental.pallas import tpu as pltpu
from jax.sharding import PartitionSpec as P

MESH = pl.DeviceIdType.MESH
F32 = jnp.float32
BF16 = jnp.bfloat16
NBLK = 64
NB = 128
NSLOT = 4
NA = 6


def bc(x):
    return jnp.broadcast_to(x, (8, 128))

def cholinv(r_ref, z_ref, lt_ref):
    G = 16
    rowi = lax.broadcasted_iota(jnp.int32, (8, 128), 0)
    lanei = lax.broadcasted_iota(jnp.int32, (8, 128), 1)
    for g in range(G):
        z_ref[8*g:8*g+8, :] = jnp.where(lanei == rowi + 8*g, 1.0, 0.0).astype(jnp.float32)
    for g in range(G):
        rg = r_ref[8*g:8*g+8, :]
        zg = z_ref[8*g:8*g+8, :]
        c = [bc(rg[:, 8*g+j:8*g+j+1]) for j in range(8)]
        m = [[bc(c[b][a:a+1, :]) for b in range(a+1)] for a in range(8)]
        rr = [None]*8
        l = [[None]*8 for _ in range(8)]
        x = [[None]*8 for _ in range(8)]
        for j in range(8):
            rr[j] = lax.rsqrt(m[j][j])
            for a in range(j+1, 8):
                l[a][j] = m[a][j]*rr[j]
            for a in range(j+1, 8):
                for b in range(j+1, a+1):
                    m[a][b] = m[a][b] - l[a][j]*l[b][j]
            x[j][j] = rr[j]
            for b in range(j):
                s = l[j][b]*x[b][b]
                for cc in range(b+1, j):
                    s = s + l[j][cc]*x[cc][b]
                x[j][b] = -(rr[j]*s)
        rb = [bc(rg[j:j+1, :]) for j in range(8)]
        zb = [bc(zg[j:j+1, :]) for j in range(8)]
        def app(vb):
            y = []
            for i in range(8):
                s = x[i][0]*vb[0]
                for j in range(1, i+1):
                    s = s + x[i][j]*vb[j]
                y.append(s)
            w = []
            for j in range(8):
                s = x[j][j]*y[j]
                for i in range(j+1, 8):
                    s = s + x[i][j]*y[i]
                w.append(s)
            return y, w
        y, w = app(rb)
        yz, wz = app(zb)
        yp, zp = y[0], yz[0]
        for i in range(1, 8):
            yp = jnp.where(rowi == i, y[i], yp)
            zp = jnp.where(rowi == i, yz[i], zp)
        lt_ref[8*g:8*g+8, :] = yp
        z_ref[8*g:8*g+8, :] = zp
        for r in range(g+1, G):
            R = r_ref[8*r:8*r+8, :]
            cr = [bc(R[:, 8*g+j:8*g+j+1]) for j in range(8)]
            t = [cr[j]*w[j] for j in range(8)]
            tz = [cr[j]*wz[j] for j in range(8)]
            while len(t) > 1:
                t = [t[i]+t[i+1] for i in range(0, len(t), 2)]
                tz = [tz[i]+tz[i+1] for i in range(0, len(tz), 2)]
            r_ref[8*r:8*r+8, :] = R - t[0]
            z_ref[8*r:8*r+8, :] = z_ref[8*r:8*r+8, :] - tz[0]


def dot_nt(a, b):
    return lax.dot_general(a, b, (((1,), (1,)), ((), ())), precision=lax.Precision.HIGHEST, preferred_element_type=F32)


def dot_bf(a, b):
    return lax.dot_general(a, b, (((1,), (1,)), ((), ())), preferred_element_type=F32)


def split3(w):
    b1 = w.astype(BF16)
    r1 = w - b1.astype(F32)
    b2 = r1.astype(BF16)
    r2 = r1 - b2.astype(F32)
    return b1, b2, r2.astype(BF16)


def kernel(a_ref, out_ref, u_ref, g_ref, ac_ref, s_ref, ud_ref, ls_ref, li_ref, lkk_ref, d_ref, lt_ref, lh_ref,
           pri_send, li_recv, ls_recv, g_send, g_recv, credit, a_loc, a_send, a_recv, o_sem):
    div, rem = lax.div, lax.rem
    p, c, r = lax.axis_index("rep"), lax.axis_index("col"), lax.axis_index("row")

    def class_of(pp, cc, rr):
        return cc + 2 * (2 * pp + rem(pp + rr, 2))

    me = class_of(p, c, r)
    flips = [(0, 1, 0), (0, 1, 1), (0, 0, 1), (1, 1, 0), (1, 1, 1), (1, 0, 0), (1, 0, 1)]

    def partner(fl):
        pp = 1 - p if fl[0] else p
        cc = 1 - c if fl[1] else c
        rr = 1 - r if fl[2] else r
        return pp, cc, rr

    def dev(fl):
        pp, cc, rr = partner(fl)
        return {"rep": pp, "col": cc, "row": rr}

    SIB, XN, YN, DG = (0, 0, 1), (0, 1, 0), (1, 0, 0), (1, 1, 0)
    groups = [SIB, XN, YN, DG]

    def xor_sib(fl):
        return (fl[0], fl[1], 1 - fl[2])

    my_q = div(me, 2)
    sib_q = div(class_of(p, c, 1 - r), 2)

    def fetch_src(col, q):
        kk = div(col, 2)
        jj, qq = div(kk, 4), rem(kk, 4)
        nat = a_ref.at[:, q, jj, qq]
        tra = a_ref.at[jj, qq, :, q]
        return nat, tra

    def fetch(col):
        slot = rem(col, NA)

        @pl.when(rem(col, 2) == r)
        def _():
            nat0, tra0 = fetch_src(col, my_q)
            nat1, tra1 = fetch_src(col, sib_q)

            @pl.when(r == c)
            def _():
                pltpu.make_async_copy(nat0, ac_ref.at[slot], a_loc.at[slot]).start()
                pltpu.make_async_remote_copy(nat1, ac_ref.at[slot], a_send.at[slot], a_recv.at[slot],
                                             device_id=dev(SIB), device_id_type=MESH).start()

            @pl.when(r != c)
            def _():
                pltpu.make_async_copy(tra0, ac_ref.at[slot], a_loc.at[slot]).start()
                pltpu.make_async_remote_copy(tra1, ac_ref.at[slot], a_send.at[slot], a_recv.at[slot],
                                             device_id=dev(SIB), device_id_type=MESH).start()

    def fetch_wait(col):
        slot = rem(col, NA)
        cp = pltpu.make_async_remote_copy(ac_ref.at[slot], ac_ref.at[slot], a_send.at[slot], a_recv.at[slot],
                                          device_id=dev(SIB), device_id_type=MESH)

        @pl.when(rem(col, 2) == r)
        def _():
            pltpu.make_async_copy(ac_ref.at[slot], ac_ref.at[slot], a_loc.at[slot]).wait()
            cp.wait_send()

        @pl.when(rem(col, 2) != r)
        def _():
            cp.wait_recv()

    zb = jnp.zeros((NB, NB), F32)
    for s in range(2):
        for h in range(2):
            ls_ref[s, h] = zb
    barrier = pltpu.get_barrier_semaphore()
    for fl in flips:
        pl.semaphore_signal(barrier, inc=1, device_id=dev(fl), device_id_type=MESH)
    pl.semaphore_wait(barrier, 7)
    for col in range(3):
        fetch(jnp.int32(col))

    def zero_u(t, _):
        u_ref[t] = jnp.zeros((1024, 256), F32)
        return 0

    lax.fori_loop(0, 32, zero_u, 0)
    for i in range(8):
        ud_ref[i] = zb
        for s in (2, 3):
            g_ref[s, me, i] = zb

    def li_copy(n, k):
        slot = rem(k, 8)
        return pltpu.make_async_remote_copy(li_ref.at[slot], li_ref.at[slot], pri_send.at[0, n], li_recv.at[slot],
                                            device_id=dev(flips[n]), device_id_type=MESH)

    def ls_copy(n, k, h):
        slot = rem(k, 8)
        return pltpu.make_async_remote_copy(ls_ref.at[slot, h], ls_ref.at[slot, h], pri_send.at[1 + h, n],
                                            ls_recv.at[slot, h], device_id=dev(flips[n]), device_id_type=MESH)

    def piece_copy(t, slot, cls, ph, via):
        src = g_ref.at[slot, cls, pl.ds(ph, 8 - ph)]
        to = SIB if via else groups[t]
        idx = 3 + t if via else t
        return pltpu.make_async_remote_copy(src, src, g_send.at[slot, idx], g_recv.at[slot, idx],
                                            device_id=dev(to), device_id_type=MESH)

    def phases(k, fn):
        for ph in range(8):
            @pl.when(div(k, 8) == ph)
            def _():
                fn(ph)

    def out_copy(m, ph, e):
        kk = div(m, 2)
        return pltpu.make_async_copy(g_ref.at[rem(m, NSLOT), 2 * e + r, pl.ds(ph, 8 - ph)],
                                     out_ref.at[pl.ds(ph, 8 - ph), e, div(kk, 4), rem(kk, 4)], o_sem.at[e])

    def step(kp1, _):
        k = kp1 - 1
        nxt = kp1

        @pl.when(nxt < NBLK)
        def _():
            fetch_wait(nxt)

        active = jnp.logical_and(k >= 0, k < NBLK)
        slot_k = rem(k + 4, NSLOT)
        slot_1 = rem(k + 3, NSLOT)
        slot_2 = rem(k + 2, NSLOT)
        k0 = jnp.maximum(k, 0)
        i_first = div(k0, 8)

        @pl.when(active)
        def _():
            own_k = rem(k, 8) == me

            @pl.when(jnp.logical_and(k >= 1, jnp.logical_not(own_k)))
            def _():
                ls_copy(0, k, 1).wait_recv()

            @pl.when(jnp.logical_and(k >= 2, jnp.logical_not(own_k)))
            def _():
                ls_copy(0, k, 0).wait_recv()

            aslot = rem(k, NA)

            @pl.when(rem(k, 2) == c)
            def _():
                def cp(i, _):
                    s_ref[i] = ac_ref[aslot, i]
                    return 0
                lax.fori_loop(i_first, 8, cp, 0)

            @pl.when(rem(k, 2) != c)
            def _():
                def cp(i, _):
                    s_ref[i] = ac_ref[aslot, i].T
                    return 0
                lax.fori_loop(i_first, 8, cp, 0)

            ls0 = ls_ref[rem(k, 8), 0]
            ls1 = ls_ref[rem(k, 8), 1]
            lane0 = pl.multiple_of(rem(k, 2) * NB, NB)

            def upd(i2, _):
                rows = pl.ds(pl.multiple_of(i2 * 256, 256), 256)
                acc = dot_nt(g_ref[slot_1, me, pl.ds(2 * i2, 2)].reshape(256, NB), ls1)
                acc = acc + dot_nt(g_ref[slot_2, me, pl.ds(2 * i2, 2)].reshape(256, NB), ls0)
                acc = acc + u_ref[div(k, 2), rows, pl.ds(lane0, NB)]
                s_ref[pl.ds(2 * i2, 2)] = s_ref[pl.ds(2 * i2, 2)] - acc.reshape(2, NB, NB)
                return 0
            lax.fori_loop(div(i_first, 2), 4, upd, 0)

            @pl.when(jnp.logical_not(own_k))
            def _():
                li_copy(0, k).wait_recv()

        @pl.when(jnp.logical_and(nxt < NBLK, rem(nxt, 8) == me))
        def _():
            i_n = div(nxt, 8)
            sl = rem(nxt, 8)
            d0 = ac_ref[rem(nxt, NA), i_n] - ud_ref[i_n]

            @pl.when(k >= 0)
            def _():
                xs = dot_nt(s_ref[i_n], li_ref[rem(k0, 8)])
                ls_ref[sl, 1] = xs
                for n in range(7):
                    ls_copy(n, nxt, 1).start()
                d_ref[...] = d0 - dot_nt(xs, xs)

            @pl.when(k < 0)
            def _():
                d_ref[...] = d0

            cholinv(d_ref, li_ref.at[sl], lt_ref)
            for n in range(7):
                li_copy(n, nxt).start()
            ri = lax.broadcasted_iota(jnp.int32, (NB, NB), 0)
            ci = lax.broadcasted_iota(jnp.int32, (NB, NB), 1)
            lkk_ref[...] = jnp.where(ri >= ci, lt_ref[...].T, 0.0)

        @pl.when(active)
        def _():
            li = li_ref[rem(k, 8)]
            lkk = lkk_ref[...]

            def solve(i, _):
                x = dot_nt(s_ref[i], li)
                gi = 8 * i + me
                x = jnp.where(gi > k, x, jnp.where(gi == k, lkk, jnp.zeros_like(x)))
                g_ref[slot_k, me, i] = x
                ud_ref[i] = ud_ref[i] + dot_nt(x, x)
                b1, b2, b3 = split3(x)
                rows = pl.ds(pl.multiple_of(i * NB, NB), NB)
                lh_ref[slot_k, rows, 0:NB] = b2
                lh_ref[slot_k, rows, NB:2 * NB] = b1
                lh_ref[slot_k, rows, 2 * NB:3 * NB] = b3
                return 0
            lax.fori_loop(i_first, 8, solve, 0)

            @pl.when(jnp.logical_and(k + 2 < NBLK, rem(k + 2, 8) == me))
            def _():
                ls_ref[rem(k + 2, 8), 0] = g_ref[slot_k, me, div(k + 2, 8)]
                for n in range(7):
                    ls_copy(n, k + 2, 0).start()

            @pl.when(rem(k, 8) == me)
            def _():
                for n in range(7):
                    li_copy(n, k).wait_send()

                @pl.when(k >= 1)
                def _():
                    for n in range(7):
                        ls_copy(n, k, 1).wait_send()

                @pl.when(k >= 2)
                def _():
                    for n in range(7):
                        ls_copy(n, k, 0).wait_send()

            @pl.when(k >= NSLOT)
            def _():
                for t in range(4):
                    pl.semaphore_wait(credit.at[t], 1)

            def send(ph):
                for t in range(4):
                    piece_copy(t, slot_k, me, ph, False).start()
            phases(k, send)

        @pl.when(jnp.logical_and(k >= 1, k <= NBLK))
        def _():
            def fwd(ph):
                for t in range(1, 4):
                    cls = class_of(*partner(groups[t]))
                    piece_copy(t, slot_1, cls, ph, False).wait_recv()
                    piece_copy(t, slot_1, cls, ph, True).start()
            phases(k - 1, fwd)

        @pl.when(k >= 2)
        def _():
            m = k - 2

            def arrive(ph):
                piece_copy(0, slot_2, class_of(*partner(SIB)), ph, False).wait_recv()
                for t in range(1, 4):
                    piece_copy(t, slot_2, class_of(*partner(xor_sib(groups[t]))), ph, True).wait_recv()

                @pl.when(rem(m, 2) == c)
                def _():
                    for e in range(4):
                        out_copy(m, ph, e).start()
            phases(m, arrive)

            for v in range(4):
                def bulk(jp, _):
                    i = div(jp, 4)
                    jc = 2 * rem(jp, 4)
                    w0 = split3(g_ref[slot_2, jc, i])
                    w1 = split3(g_ref[slot_2, jc + 1, i])
                    b1, b2, b3 = [jnp.concatenate([x0, x1], axis=0) for x0, x1 in zip(w0, w1)]
                    r1 = jnp.concatenate([b1, b1], axis=1)
                    r2 = jnp.concatenate([b2, b2], axis=1)
                    r3 = jnp.concatenate([b3, b1], axis=1)
                    for ch in range(v, 4):
                        rows = pl.ds(ch * 256, 256)
                        l12 = lh_ref[slot_2, rows, 0:256]
                        l13 = lh_ref[slot_2, rows, 128:384]
                        acc = dot_bf(l12, r1) + dot_bf(l12, r2) + dot_bf(l13, r3)
                        u_ref[jp, rows, :] = u_ref[jp, rows, :] + acc
                    return 0
                lax.fori_loop(jnp.maximum(div(m + 3, 2), 8 * v), 8 * v + 8, bulk, 0)

            def finish(ph):
                for t in range(4):
                    piece_copy(t, slot_2, me, ph, False).wait_send()
                for t in range(1, 4):
                    piece_copy(t, slot_2, class_of(*partner(groups[t])), ph, True).wait_send()

                @pl.when(rem(m, 2) == c)
                def _():
                    for e in range(4):
                        out_copy(m, ph, e).wait()
            phases(m, finish)

            @pl.when(m + NSLOT < NBLK)
            def _():
                for t in range(4):
                    pl.semaphore_signal(credit.at[t], inc=1, device_id=dev(groups[t]), device_id_type=MESH)

        @pl.when(k + 4 < NBLK)
        def _():
            fetch(k + 4)
        return 0

    lax.fori_loop(0, NBLK + 3, step, 0)


def solution(mesh):
    grid_spec = P(("b", "row"), "col")

    def local_factor(a_loc):
        a6 = a_loc.reshape(8, 4, 8, 4, NB, NB)
        dma = pltpu.SemaphoreType.DMA
        fac = pl.pallas_call(
            kernel,
            out_shape=jax.ShapeDtypeStruct((8, 4, 8, 4, NB, NB), F32),
            in_specs=[pl.BlockSpec(memory_space=pl.ANY)],
            out_specs=pl.BlockSpec(memory_space=pl.ANY),
            scratch_shapes=[
                pltpu.VMEM((32, 1024, 256), F32),
                pltpu.VMEM((NSLOT, 8, 8, NB, NB), F32),
                pltpu.VMEM((NA, 8, NB, NB), F32),
                pltpu.VMEM((8, NB, NB), F32),
                pltpu.VMEM((8, NB, NB), F32),
                pltpu.VMEM((8, 2, NB, NB), F32),
                pltpu.VMEM((8, NB, NB), F32),
                pltpu.VMEM((NB, NB), F32),
                pltpu.VMEM((NB, NB), F32),
                pltpu.VMEM((NB, NB), F32),
                pltpu.VMEM((NSLOT, 1024, 384), BF16),
                dma((3, 7)),
                dma((8,)),
                dma((8, 2)),
                dma((NSLOT, 7)),
                dma((NSLOT, 7)),
                pltpu.SemaphoreType.REGULAR((4,)),
                dma((NA,)),
                dma((NA,)),
                dma((NA,)),
                dma((4,)),
            ],
            compiler_params=pltpu.CompilerParams(
                collective_id=0, has_side_effects=True, vmem_limit_bytes=67043328),
            name="chol_all",
        )(a6)
        fac = fac.reshape(32, 32, NB, NB)
        gi = 2 * jnp.arange(32) + lax.axis_index("row")
        gj = 2 * jnp.arange(32) + lax.axis_index("col")
        keep = gi[:, None] >= gj[None, :]
        return jnp.where(keep[:, :, None, None], fac, 0.0)

    return jax.shard_map(local_factor, mesh=mesh, in_specs=grid_spec, out_specs=grid_spec, check_vma=False)
```

```python
import jax
import jax.numpy as jnp
from jax import lax
from jax.experimental import pallas as pl
from jax.experimental.pallas import tpu as pltpu
from jax.sharding import PartitionSpec as P

MESH = pl.DeviceIdType.MESH
F32 = jnp.float32
BF16 = jnp.bfloat16
NBLK = 64
NB = 128
NSLOT = 4
NA = 6


def bc(x):
    return jnp.broadcast_to(x, (8, 128))

def cholinv(r_ref, z_ref, lt_ref):
    G = 16
    rowi = lax.broadcasted_iota(jnp.int32, (8, 128), 0)
    lanei = lax.broadcasted_iota(jnp.int32, (8, 128), 1)
    for g in range(G):
        z_ref[8*g:8*g+8, :] = jnp.where(lanei == rowi + 8*g, 1.0, 0.0).astype(jnp.float32)
    for g in range(G):
        rg = r_ref[8*g:8*g+8, :]
        zg = z_ref[8*g:8*g+8, :]
        c = [bc(rg[:, 8*g+j:8*g+j+1]) for j in range(8)]
        m = [[bc(c[b][a:a+1, :]) for b in range(a+1)] for a in range(8)]
        rr = [None]*8
        l = [[None]*8 for _ in range(8)]
        x = [[None]*8 for _ in range(8)]
        for j in range(8):
            rr[j] = lax.rsqrt(m[j][j])
            for a in range(j+1, 8):
                l[a][j] = m[a][j]*rr[j]
            for a in range(j+1, 8):
                for b in range(j+1, a+1):
                    m[a][b] = m[a][b] - l[a][j]*l[b][j]
            x[j][j] = rr[j]
            for b in range(j):
                s = l[j][b]*x[b][b]
                for cc in range(b+1, j):
                    s = s + l[j][cc]*x[cc][b]
                x[j][b] = -(rr[j]*s)
        rb = [bc(rg[j:j+1, :]) for j in range(8)]
        zb = [bc(zg[j:j+1, :]) for j in range(8)]
        def app(vb):
            y = []
            for i in range(8):
                s = x[i][0]*vb[0]
                for j in range(1, i+1):
                    s = s + x[i][j]*vb[j]
                y.append(s)
            w = []
            for j in range(8):
                s = x[j][j]*y[j]
                for i in range(j+1, 8):
                    s = s + x[i][j]*y[i]
                w.append(s)
            return y, w
        y, w = app(rb)
        yz, wz = app(zb)
        yp, zp = y[0], yz[0]
        for i in range(1, 8):
            yp = jnp.where(rowi == i, y[i], yp)
            zp = jnp.where(rowi == i, yz[i], zp)
        lt_ref[8*g:8*g+8, :] = yp
        z_ref[8*g:8*g+8, :] = zp
        for r in range(g+1, G):
            R = r_ref[8*r:8*r+8, :]
            cr = [bc(R[:, 8*g+j:8*g+j+1]) for j in range(8)]
            t = [cr[j]*w[j] for j in range(8)]
            tz = [cr[j]*wz[j] for j in range(8)]
            while len(t) > 1:
                t = [t[i]+t[i+1] for i in range(0, len(t), 2)]
                tz = [tz[i]+tz[i+1] for i in range(0, len(tz), 2)]
            r_ref[8*r:8*r+8, :] = R - t[0]
            z_ref[8*r:8*r+8, :] = z_ref[8*r:8*r+8, :] - tz[0]


def dot_nt(a, b):
    return lax.dot_general(a, b, (((1,), (1,)), ((), ())), precision=lax.Precision.HIGHEST, preferred_element_type=F32)


def dot_bf(a, b):
    return lax.dot_general(a, b, (((1,), (1,)), ((), ())), preferred_element_type=F32)


def split3(w):
    b1 = w.astype(BF16)
    r1 = w - b1.astype(F32)
    b2 = r1.astype(BF16)
    r2 = r1 - b2.astype(F32)
    return b1, b2, r2.astype(BF16)


def dot6(lhs, rhs):
    b1, b2, b3 = rhs
    acc = dot_bf(lhs[:, 0:256], jnp.concatenate([b1, b1], axis=1))
    acc = acc + dot_bf(lhs[:, 0:256], jnp.concatenate([b2, b2], axis=1))
    return acc + dot_bf(lhs[:, 128:384], jnp.concatenate([b3, b1], axis=1))


def parts_lhs(x):
    b1, b2, b3 = split3(x)
    return jnp.concatenate([b2, b1, b3], axis=1)


def kernel(a_ref, out_ref, u_ref, g_ref, ac_ref, s_ref, ls_ref, li_ref, lkk_ref, d_ref, lt_ref, lh_ref,
           pri_send, li_recv, ls_recv, g_send, g_recv, credit, a_loc, a_send, a_recv, o_sem):
    div, rem = lax.div, lax.rem
    p, c, r = lax.axis_index("rep"), lax.axis_index("col"), lax.axis_index("row")

    def class_of(pp, cc, rr):
        return cc + 2 * (2 * pp + rem(pp + rr, 2))

    me = class_of(p, c, r)
    flips = [(0, 1, 0), (0, 1, 1), (0, 0, 1), (1, 1, 0), (1, 1, 1), (1, 0, 0), (1, 0, 1)]

    def partner(fl):
        pp = 1 - p if fl[0] else p
        cc = 1 - c if fl[1] else c
        rr = 1 - r if fl[2] else r
        return pp, cc, rr

    def dev(fl):
        pp, cc, rr = partner(fl)
        return {"rep": pp, "col": cc, "row": rr}

    SIB, XN, YN, DG = (0, 0, 1), (0, 1, 0), (1, 0, 0), (1, 1, 0)
    groups = [SIB, XN, YN, DG]

    def xor_sib(fl):
        return (fl[0], fl[1], 1 - fl[2])

    my_q = div(me, 2)
    sib_q = div(class_of(p, c, 1 - r), 2)

    def fetch_src(col, q):
        kk = div(col, 2)
        jj, qq = div(kk, 4), rem(kk, 4)
        nat = a_ref.at[:, q, jj, qq]
        tra = a_ref.at[jj, qq, :, q]
        return nat, tra

    def fetch(col):
        slot = rem(col, NA)

        @pl.when(rem(col, 2) == r)
        def _():
            nat0, tra0 = fetch_src(col, my_q)
            nat1, tra1 = fetch_src(col, sib_q)

            @pl.when(r == c)
            def _():
                pltpu.make_async_copy(nat0, ac_ref.at[slot], a_loc.at[slot]).start()
                pltpu.make_async_remote_copy(nat1, ac_ref.at[slot], a_send.at[slot], a_recv.at[slot],
                                             device_id=dev(SIB), device_id_type=MESH).start()

            @pl.when(r != c)
            def _():
                pltpu.make_async_copy(tra0, ac_ref.at[slot], a_loc.at[slot]).start()
                pltpu.make_async_remote_copy(tra1, ac_ref.at[slot], a_send.at[slot], a_recv.at[slot],
                                             device_id=dev(SIB), device_id_type=MESH).start()

    def fetch_wait(col):
        slot = rem(col, NA)
        cp = pltpu.make_async_remote_copy(ac_ref.at[slot], ac_ref.at[slot], a_send.at[slot], a_recv.at[slot],
                                          device_id=dev(SIB), device_id_type=MESH)

        @pl.when(rem(col, 2) == r)
        def _():
            pltpu.make_async_copy(ac_ref.at[slot], ac_ref.at[slot], a_loc.at[slot]).wait()
            cp.wait_send()

        @pl.when(rem(col, 2) != r)
        def _():
            cp.wait_recv()

    zb = jnp.zeros((NB, NB), F32)
    for s in range(2):
        for h in range(2):
            ls_ref[s, h] = zb
    barrier = pltpu.get_barrier_semaphore()
    for fl in flips:
        pl.semaphore_signal(barrier, inc=1, device_id=dev(fl), device_id_type=MESH)
    pl.semaphore_wait(barrier, 7)
    for col in range(3):
        fetch(jnp.int32(col))

    def zero_u(t, _):
        u_ref[t] = jnp.zeros((1024, 256), F32)
        return 0

    lax.fori_loop(0, 32, zero_u, 0)
    for s in (2, 3):
        lh_ref[s] = jnp.zeros((1024, 384), BF16)
        for i in range(8):
            g_ref[s, me, i] = zb

    def pri_dev(n, k):
        if n == 3:
            return dev(SIB)
        pp, cc, _ = partner([XN, DG, YN][n])
        rr = jnp.where(rem(k, 4) == 1, 1 - r, r)
        return {"rep": pp, "col": cc, "row": rr}

    def li_copy(n, k):
        slot = rem(k, 8)
        return pltpu.make_async_remote_copy(li_ref.at[slot], li_ref.at[slot], pri_send.at[0, n], li_recv.at[slot],
                                            device_id=pri_dev(n, k), device_id_type=MESH)

    def ls_copy(n, k, h):
        slot = rem(k, 8)
        return pltpu.make_async_remote_copy(ls_ref.at[slot, h], ls_ref.at[slot, h], pri_send.at[1 + h, n],
                                            ls_recv.at[slot, h], device_id=pri_dev(n, k), device_id_type=MESH)

    def hands_on(k):
        q_o = rem(div(k, 2), 4)
        p_o = div(q_o, 2)
        r_o = rem(q_o + p_o, 2)
        turn = jnp.where(rem(k, 4) == 1, 1, 0)
        away = jnp.logical_or(p != p_o, c != rem(k, 2))
        return jnp.logical_and(away, r == rem(r_o + turn, 2))

    def piece_copy(t, slot, cls, ph, via):
        src = g_ref.at[slot, cls, pl.ds(ph, 8 - ph)]
        to = SIB if via else groups[t]
        idx = 3 + t if via else t
        return pltpu.make_async_remote_copy(src, src, g_send.at[slot, idx], g_recv.at[slot, idx],
                                            device_id=dev(to), device_id_type=MESH)

    def relay_copy(slot, cls, ph, to):
        src = g_ref.at[slot, cls, pl.ds(ph, 8 - ph)]
        return pltpu.make_async_remote_copy(src, src, g_send.at[slot, 3], g_recv.at[slot, 3],
                                            device_id=dev(to), device_id_type=MESH)

    def first_of(k, cls):
        return div(k - cls + 7, 8)

    def phases(k, cls, fn):
        for ph in range(8):
            @pl.when(first_of(k, cls) == ph)
            def _():
                fn(ph)

    def out_copy(m, ph, e):
        kk = div(m, 2)
        return pltpu.make_async_copy(g_ref.at[rem(m, NSLOT), 2 * e + r, pl.ds(ph, 8 - ph)],
                                     out_ref.at[pl.ds(ph, 8 - ph), e, div(kk, 4), rem(kk, 4)], o_sem.at[e])

    def step(kp1, _):
        k = kp1 - 1
        nxt = kp1

        @pl.when(nxt < NBLK)
        def _():
            fetch_wait(nxt)

        active = jnp.logical_and(k >= 0, k < NBLK)
        slot_k = rem(k + 4, NSLOT)
        slot_1 = rem(k + 3, NSLOT)
        slot_2 = rem(k + 2, NSLOT)
        k0 = jnp.maximum(k, 0)

        @pl.when(active)
        def _():
            own_k = rem(k, 8) == me

            hand = hands_on(k)
            for h in (0, 1):
                @pl.when(jnp.logical_and(k >= 2 - h, jnp.logical_not(own_k)))
                def _():
                    ls_copy(3, k, h).wait_recv()

                    @pl.when(hand)
                    def _():
                        ls_copy(3, k, h).start()

            aslot = rem(k, NA)
            ls0 = split3(ls_ref[rem(k, 8), 0])
            ls1 = split3(ls_ref[rem(k, 8), 1])
            lane0 = pl.multiple_of(rem(k, 2) * NB, NB)

            def update(ph):
                n = 1024 - NB * ph
                rows = pl.ds(NB * ph, n)

                @pl.when(rem(k, 2) == c)
                def _():
                    s_ref[rows, :] = ac_ref[aslot, ph:8].reshape(n, NB)

                @pl.when(rem(k, 2) != c)
                def _():
                    for i in range(ph, 8):
                        s_ref[i * NB:(i + 1) * NB, :] = ac_ref[aslot, i].T

                acc = dot6(lh_ref[slot_1, rows, :], ls1) + dot6(lh_ref[slot_2, rows, :], ls0)
                s_ref[rows, :] = s_ref[rows, :] - (u_ref[div(k, 2), rows, pl.ds(lane0, NB)] + acc)
            phases(k, me, update)

            @pl.when(jnp.logical_and(nxt < NBLK, rem(nxt, 8) == me))
            def _():
                i_n = div(nxt, 8)
                lane_n = pl.multiple_of(rem(nxt, 2) * NB, NB)
                rows_n = pl.ds(pl.multiple_of(i_n * NB, NB), NB)
                p1 = g_ref[slot_1, me, i_n]
                p2 = g_ref[slot_2, me, i_n]
                d_ref[...] = (ac_ref[rem(nxt, NA), i_n] - u_ref[div(nxt, 2), rows_n, pl.ds(lane_n, NB)]
                              - (dot_nt(p1, p1) + dot_nt(p2, p2)))

            @pl.when(jnp.logical_not(own_k))
            def _():
                li_copy(3, k).wait_recv()

                @pl.when(hand)
                def _():
                    li_copy(3, k).start()

        @pl.when(jnp.logical_and(nxt < NBLK, rem(nxt, 8) == me))
        def _():
            i_n = div(nxt, 8)
            sl = rem(nxt, 8)
            rows_n = pl.ds(pl.multiple_of(i_n * NB, NB), NB)

            @pl.when(k < 0)
            def _():
                d_ref[...] = ac_ref[0, 0]

            @pl.when(k >= 0)
            def _():
                xs = dot_nt(s_ref[rows_n, :], li_ref[rem(k0, 8)])
                ls_ref[sl, 1] = xs
                for n in range(4):
                    ls_copy(n, nxt, 1).start()
                d_ref[...] = d_ref[...] - dot_nt(xs, xs)

            cholinv(d_ref, li_ref.at[sl], lt_ref)
            for n in range(4):
                li_copy(n, nxt).start()
            ri = lax.broadcasted_iota(jnp.int32, (NB, NB), 0)
            ci = lax.broadcasted_iota(jnp.int32, (NB, NB), 1)
            lkk_ref[...] = jnp.where(ri >= ci, lt_ref[...].T, 0.0)

        @pl.when(active)
        def _():
            li = li_ref[rem(k, 8)]
            lkk = lkk_ref[...]

            li3 = split3(li)

            def solve(ph):
                n = 1024 - NB * ph
                rows = pl.ds(NB * ph, n)
                x = dot6(parts_lhs(s_ref[rows, :]), li3)
                g_ref[slot_k, me, ph:8] = x.reshape(8 - ph, NB, NB)
                lh_ref[slot_k, rows, :] = parts_lhs(x)

                @pl.when(8 * ph + me == k)
                def _():
                    g_ref[slot_k, me, ph] = lkk
            phases(k, me, solve)

            @pl.when(jnp.logical_and(k + 2 < NBLK, rem(k + 2, 8) == me))
            def _():
                ls_ref[rem(k + 2, 8), 0] = g_ref[slot_k, me, div(k + 2, 8)]
                for n in range(4):
                    ls_copy(n, k + 2, 0).start()

            for n in range(4):
                sent = rem(k, 8) == me
                if n == 3:
                    sent = jnp.logical_or(sent, hands_on(k))

                @pl.when(sent)
                def _():
                    li_copy(n, k).wait_send()
                for h in (0, 1):
                    @pl.when(jnp.logical_and(sent, k >= 2 - h))
                    def _():
                        ls_copy(n, k, h).wait_send()

            @pl.when(k >= NSLOT)
            def _():
                for t in range(3):
                    pl.semaphore_wait(credit.at[t], 1)

            def send(ph):
                for t in range(3):
                    piece_copy(t, slot_k, me, ph, False).start()
            phases(k, me, send)

        @pl.when(jnp.logical_and(k >= 1, k <= NBLK))
        def _():
            for t, to, odd in ((1, YN, 0), (2, XN, 1)):
                cls = class_of(*partner(groups[t]))

                def fwd(ph):
                    piece_copy(t, slot_1, cls, ph, False).wait_recv()
                    piece_copy(t, slot_1, cls, ph, True).start()

                    @pl.when(rem(k - 1, 2) == odd)
                    def _():
                        relay_copy(slot_1, cls, ph, to).start()
                phases(k - 1, cls, fwd)

        @pl.when(k >= 2)
        def _():
            m = k - 2
            dg_cls = class_of(*partner(DG))

            def fwd_dg(ph):
                piece_copy(3, slot_2, dg_cls, ph, False).wait_recv()
                piece_copy(3, slot_2, dg_cls, ph, True).start()
            phases(m, dg_cls, fwd_dg)

            sib_cls = class_of(*partner(SIB))
            phases(m, sib_cls, lambda ph: piece_copy(0, slot_2, sib_cls, ph, False).wait_recv())
            for t in range(1, 4):
                cls = class_of(*partner(xor_sib(groups[t])))
                phases(m, cls, lambda ph: piece_copy(t, slot_2, cls, ph, True).wait_recv())

            @pl.when(rem(m, 2) == c)
            def _():
                for e in range(4):
                    phases(m, 2 * e + r, lambda ph: out_copy(m, ph, e).start())

            start = div(m + 3, 2)
            for v in range(8):
                rows = pl.ds(NB * v, 1024 - NB * v)

                def bulk(jp, v=v, rows=rows):
                    jc = 2 * rem(jp, 4)
                    w0 = split3(g_ref[slot_2, jc, v])
                    w1 = split3(g_ref[slot_2, jc + 1, v])
                    w = [jnp.concatenate([x0, x1], axis=0) for x0, x1 in zip(w0, w1)]
                    u_ref[jp, rows, :] = u_ref[jp, rows, :] + dot6(lh_ref[slot_2, rows, :], w)

                @pl.when(start <= 4 * v)
                def _():
                    for q in range(4):
                        bulk(4 * v + q)

                @pl.when(jnp.logical_and(start > 4 * v, start < 4 * v + 4))
                def _():
                    def one(jp, _):
                        bulk(jp)
                        return 0
                    lax.fori_loop(start, 4 * v + 4, one, 0)

            def finish(ph):
                for t in range(3):
                    piece_copy(t, slot_2, me, ph, False).wait_send()
            phases(m, me, finish)
            for t in range(1, 4):
                cls = class_of(*partner(groups[t]))

                def finish_fwd(ph):
                    piece_copy(t, slot_2, cls, ph, True).wait_send()
                    if t < 3:
                        @pl.when(rem(m, 2) == t - 1)
                        def _():
                            relay_copy(slot_2, cls, ph, YN).wait_send()
                phases(m, cls, finish_fwd)

            @pl.when(rem(m, 2) == c)
            def _():
                for e in range(4):
                    phases(m, 2 * e + r, lambda ph: out_copy(m, ph, e).wait())

            @pl.when(m + NSLOT < NBLK)
            def _():
                for t in range(3):
                    pl.semaphore_signal(credit.at[t], inc=1, device_id=dev(groups[t]), device_id_type=MESH)

        @pl.when(k + 4 < NBLK)
        def _():
            fetch(k + 4)
        return 0

    lax.fori_loop(0, NBLK + 3, step, 0)


def solution(mesh):
    grid_spec = P(("b", "row"), "col")

    def local_factor(a_loc):
        a6 = a_loc.reshape(8, 4, 8, 4, NB, NB)
        dma = pltpu.SemaphoreType.DMA
        fac = pl.pallas_call(
            kernel,
            out_shape=jax.ShapeDtypeStruct((8, 4, 8, 4, NB, NB), F32),
            in_specs=[pl.BlockSpec(memory_space=pl.ANY)],
            out_specs=pl.BlockSpec(memory_space=pl.ANY),
            scratch_shapes=[
                pltpu.VMEM((32, 1024, 256), F32),
                pltpu.VMEM((NSLOT, 8, 8, NB, NB), F32),
                pltpu.VMEM((NA, 8, NB, NB), F32),
                pltpu.VMEM((1024, NB), F32),
                pltpu.VMEM((8, 2, NB, NB), F32),
                pltpu.VMEM((8, NB, NB), F32),
                pltpu.VMEM((NB, NB), F32),
                pltpu.VMEM((NB, NB), F32),
                pltpu.VMEM((NB, NB), F32),
                pltpu.VMEM((NSLOT, 1024, 384), BF16),
                dma((3, 4)),
                dma((8,)),
                dma((8, 2)),
                dma((NSLOT, 7)),
                dma((NSLOT, 7)),
                pltpu.SemaphoreType.REGULAR((3,)),
                dma((NA,)),
                dma((NA,)),
                dma((NA,)),
                dma((4,)),
            ],
            compiler_params=pltpu.CompilerParams(
                collective_id=0, has_side_effects=True, vmem_limit_bytes=67043328),
            name="chol_all",
        )(a6)
        fac = fac.reshape(32, 32, NB, NB)
        gi = 2 * jnp.arange(32) + lax.axis_index("row")
        gj = 2 * jnp.arange(32) + lax.axis_index("col")
        keep = gi[:, None] >= gj[None, :]
        return jnp.where(keep[:, :, None, None], fac, 0.0)

    return jax.shard_map(local_factor, mesh=mesh, in_specs=grid_spec, out_specs=grid_spec, check_vma=False)
```

```python
import jax
import jax.numpy as jnp
from jax import lax
from jax.experimental import pallas as pl
from jax.experimental.pallas import tpu as pltpu
from jax.sharding import PartitionSpec as P

MESH = pl.DeviceIdType.MESH
F32 = jnp.float32
BF16 = jnp.bfloat16
NBLK = 64
NB = 128
NSLOT = 4
NA = 6
NP = 16


def bc(x):
    return jnp.broadcast_to(x, (8, 128))

def cholinv(r_ref, z_ref, lt_ref):
    G = 16
    rowi = lax.broadcasted_iota(jnp.int32, (8, 128), 0)
    lanei = lax.broadcasted_iota(jnp.int32, (8, 128), 1)
    for g in range(G):
        z_ref[8*g:8*g+8, :] = jnp.where(lanei == rowi + 8*g, 1.0, 0.0).astype(jnp.float32)
    for g in range(G):
        rg = r_ref[8*g:8*g+8, :]
        zg = z_ref[8*g:8*g+8, :]
        c = [bc(rg[:, 8*g+j:8*g+j+1]) for j in range(8)]
        m = [[bc(c[b][a:a+1, :]) for b in range(a+1)] for a in range(8)]
        rr = [None]*8
        l = [[None]*8 for _ in range(8)]
        x = [[None]*8 for _ in range(8)]
        for j in range(8):
            rr[j] = lax.rsqrt(m[j][j])
            for a in range(j+1, 8):
                l[a][j] = m[a][j]*rr[j]
            for a in range(j+1, 8):
                for b in range(j+1, a+1):
                    m[a][b] = m[a][b] - l[a][j]*l[b][j]
            x[j][j] = rr[j]
            for b in range(j):
                s = l[j][b]*x[b][b]
                for cc in range(b+1, j):
                    s = s + l[j][cc]*x[cc][b]
                x[j][b] = -(rr[j]*s)
        rb = [bc(rg[j:j+1, :]) for j in range(8)]
        zb = [bc(zg[j:j+1, :]) for j in range(8)]

        def app(vb):
            y = []
            for i in range(8):
                s = vb[i]
                for j in range(i):
                    s = s - l[i][j]*y[j]
                y.append(s*rr[i])
            w = []
            for j in range(8):
                s = x[j][j]*y[j]
                for i in range(j+1, 8):
                    s = s + x[i][j]*y[i]
                w.append(s)
            return y, w
        y, w = app(rb)
        yz, wz = app(zb)
        yp, zp = y[0], yz[0]
        for i in range(1, 8):
            yp = jnp.where(rowi == i, y[i], yp)
            zp = jnp.where(rowi == i, yz[i], zp)
        lt_ref[8*g:8*g+8, :] = yp
        z_ref[8*g:8*g+8, :] = zp
        for r in range(g+1, G):
            R = r_ref[8*r:8*r+8, :]
            cr = [bc(R[:, 8*g+j:8*g+j+1]) for j in range(8)]
            t = [cr[j]*w[j] for j in range(8)]
            tz = [cr[j]*wz[j] for j in range(8)]
            while len(t) > 1:
                t = [t[i]+t[i+1] for i in range(0, len(t), 2)]
                tz = [tz[i]+tz[i+1] for i in range(0, len(tz), 2)]
            r_ref[8*r:8*r+8, :] = R - t[0]
            z_ref[8*r:8*r+8, :] = z_ref[8*r:8*r+8, :] - tz[0]


def dot_nt(a, b):
    return lax.dot_general(a, b, (((1,), (1,)), ((), ())), precision=lax.Precision.HIGHEST, preferred_element_type=F32)


def dot_bf(a, b):
    return lax.dot_general(a, b, (((1,), (1,)), ((), ())), preferred_element_type=F32)


def split3(w):
    b1 = w.astype(BF16)
    r1 = w - b1.astype(F32)
    b2 = r1.astype(BF16)
    r2 = r1 - b2.astype(F32)
    return b1, b2, r2.astype(BF16)


def dot6(lhs, rhs):
    b1, b2, b3 = rhs
    acc = dot_bf(lhs[:, 0:256], jnp.concatenate([b1, b1], axis=1))
    acc = acc + dot_bf(lhs[:, 0:256], jnp.concatenate([b2, b2], axis=1))
    return acc + dot_bf(lhs[:, 128:384], jnp.concatenate([b3, b1], axis=1))


def parts_lhs(x):
    b1, b2, b3 = split3(x)
    return jnp.concatenate([b2, b1, b3], axis=1)


def kernel(a_ref, out_ref, u_ref, g_ref, ac_ref, s_ref, ls_ref, li_ref, lkk_ref, d_ref, lt_ref, lh_ref,
           pri_send, li_recv, ls_recv, g_send, g_recv, credit, a_loc, a_send, a_recv, o_sem,
           o3_sem, lk_send, lk_recv, a_free):
    div, rem = lax.div, lax.rem
    p, c, r = lax.axis_index("rep"), lax.axis_index("col"), lax.axis_index("row")

    def class_of(pp, cc, rr):
        return cc + 2 * (2 * pp + rem(pp + rr, 2))

    me = class_of(p, c, r)
    flips = [(0, 1, 0), (0, 1, 1), (0, 0, 1), (1, 1, 0), (1, 1, 1), (1, 0, 0), (1, 0, 1)]

    def partner(fl):
        pp = 1 - p if fl[0] else p
        cc = 1 - c if fl[1] else c
        rr = 1 - r if fl[2] else r
        return pp, cc, rr

    def dev(fl):
        pp, cc, rr = partner(fl)
        return {"rep": pp, "col": cc, "row": rr}

    SIB, XN, YN, DG = (0, 0, 1), (0, 1, 0), (1, 0, 0), (1, 1, 0)
    groups = [SIB, XN, YN, DG]

    def xor_sib(fl):
        return (fl[0], fl[1], 1 - fl[2])

    my_q = div(me, 2)
    sib_q = div(class_of(p, c, 1 - r), 2)

    def fetch_src(col, q):
        kk = div(col, 2)
        jj, qq = div(kk, 4), rem(kk, 4)
        nat = a_ref.at[:, q, jj, qq]
        tra = a_ref.at[jj, qq, :, q]
        return nat, tra

    def fetch(col):
        slot = rem(col, NA)

        @pl.when(rem(col, 2) == r)
        def _():
            nat0, tra0 = fetch_src(col, my_q)
            nat1, tra1 = fetch_src(col, sib_q)

            @pl.when(r == c)
            def _():
                pltpu.make_async_copy(nat0, ac_ref.at[slot], a_loc.at[slot]).start()
                pltpu.make_async_remote_copy(nat1, ac_ref.at[slot], a_send.at[slot], a_recv.at[slot],
                                             device_id=dev(SIB), device_id_type=MESH).start()

            @pl.when(r != c)
            def _():
                pltpu.make_async_copy(tra0, ac_ref.at[slot], a_loc.at[slot]).start()
                pltpu.make_async_remote_copy(tra1, ac_ref.at[slot], a_send.at[slot], a_recv.at[slot],
                                             device_id=dev(SIB), device_id_type=MESH).start()

    def fetch_wait(col):
        slot = rem(col, NA)
        cp = pltpu.make_async_remote_copy(ac_ref.at[slot], ac_ref.at[slot], a_send.at[slot], a_recv.at[slot],
                                          device_id=dev(SIB), device_id_type=MESH)

        @pl.when(rem(col, 2) == r)
        def _():
            pltpu.make_async_copy(ac_ref.at[slot], ac_ref.at[slot], a_loc.at[slot]).wait()
            cp.wait_send()

        @pl.when(rem(col, 2) != r)
        def _():
            cp.wait_recv()

    zb = jnp.zeros((NB, NB), F32)
    for s in range(2):
        for h in range(2):
            ls_ref[s, h] = zb
    barrier = pltpu.get_barrier_semaphore()
    for fl in flips:
        pl.semaphore_signal(barrier, inc=1, device_id=dev(fl), device_id_type=MESH)
    pl.semaphore_wait(barrier, 7)
    for col in range(3):
        fetch(jnp.int32(col))

    def zero_u(t, _):
        u_ref[t] = jnp.zeros((1024, 256), F32)
        return 0

    lax.fori_loop(0, 32, zero_u, 0)
    for s in (2, 3):
        lh_ref[s] = jnp.zeros((1024, 384), BF16)
        for i in range(8):
            g_ref[s, me, i] = zb

    def pri_dev(n, k):
        if n == 3:
            return dev(SIB)
        pp, cc, _ = partner([XN, DG, YN][n])
        rr = jnp.where(rem(k, 4) == 1, 1 - r, r)
        return {"rep": pp, "col": cc, "row": rr}

    def li_copy(n, k):
        slot = rem(k, NP)
        return pltpu.make_async_remote_copy(li_ref.at[slot], li_ref.at[slot], pri_send.at[0, n], li_recv.at[slot],
                                            device_id=pri_dev(n, k), device_id_type=MESH)

    def ls_copy(n, k, h):
        slot = rem(k, NP)
        return pltpu.make_async_remote_copy(ls_ref.at[slot, h], ls_ref.at[slot, h], pri_send.at[1 + h, n],
                                            ls_recv.at[slot, h], device_id=pri_dev(n, k), device_id_type=MESH)

    def lk_copy(n, k):
        slot = rem(k, NP)
        to = {"rep": p if n == 0 else 1 - p, "col": c, "row": c}
        return pltpu.make_async_remote_copy(lkk_ref.at[slot], lkk_ref.at[slot], lk_send.at[n], lk_recv.at[slot],
                                            device_id=to, device_id_type=MESH)

    def row_copy(n, k):
        src = [ls_ref.at[rem(k, NP), 0], ls_ref.at[rem(k, NP), 1], lkk_ref.at[rem(k, NP)]][n]
        kk = div(k - [2, 1, 0][n], 2)
        return pltpu.make_async_copy(src, out_ref.at[div(k, 8), div(rem(k, 8), 2), div(kk, 4), rem(kk, 4)], o3_sem.at[n])

    def row_outs(k, fn):
        @pl.when(jnp.logical_and(rem(k, 2) == r, c != r))
        def _():
            @pl.when(k >= 1)
            def _():
                fn(1)

        @pl.when(jnp.logical_and(rem(k, 2) == r, c == r))
        def _():
            fn(2)

            @pl.when(k >= 2)
            def _():
                fn(0)

    def hands_on(k):
        q_o = rem(div(k, 2), 4)
        p_o = div(q_o, 2)
        r_o = rem(q_o + p_o, 2)
        turn = jnp.where(rem(k, 4) == 1, 1, 0)
        away = jnp.logical_or(p != p_o, c != rem(k, 2))
        return jnp.logical_and(away, r == rem(r_o + turn, 2))

    def piece_copy(t, slot, cls, ph, via):
        src = g_ref.at[slot, cls, pl.ds(ph, 8 - ph)]
        to = SIB if via else groups[t]
        idx = 3 + t if via else t
        return pltpu.make_async_remote_copy(src, src, g_send.at[slot, idx], g_recv.at[slot, idx],
                                            device_id=dev(to), device_id_type=MESH)

    def relay_copy(slot, cls, ph, h, t):
        lo, hi = (ph, ph + h) if t == 1 else (ph + h, 8)
        src = g_ref.at[slot, cls, pl.ds(lo, hi - lo)]
        idx = 3 if t == 1 else 7
        return pltpu.make_async_remote_copy(src, src, g_send.at[slot, idx], g_recv.at[slot, idx],
                                            device_id=dev(YN if t == 1 else XN), device_id_type=MESH)

    def relay(k, slot, cls, ph, t, fn):
        n = 8 - ph
        if n % 2 == 0:
            fn(relay_copy(slot, cls, ph, n // 2, t))
        else:
            for par in (0, 1):
                h = (n + par) // 2
                if (h if t == 1 else n - h) > 0:
                    @pl.when(rem(k, 2) == par)
                    def _():
                        fn(relay_copy(slot, cls, ph, h, t))

    def first_of(k, cls):
        return div(k - cls + 7, 8)

    def phases(k, cls, fn):
        for ph in range(8):
            @pl.when(first_of(k, cls) == ph)
            def _():
                fn(ph)

    def out_copy(m, ph, e):
        kk = div(m, 2)
        return pltpu.make_async_copy(g_ref.at[rem(m, NSLOT), 2 * e + r, pl.ds(ph, 8 - ph)],
                                     out_ref.at[pl.ds(ph, 8 - ph), e, div(kk, 4), rem(kk, 4)], o_sem.at[e])

    def step(kp1, _):
        k = kp1 - 1
        nxt = kp1

        @pl.when(nxt < NBLK)
        def _():
            fetch_wait(nxt)

        active = jnp.logical_and(k >= 0, k < NBLK)
        slot_k = rem(k + 4, NSLOT)
        slot_1 = rem(k + 3, NSLOT)
        slot_2 = rem(k + 2, NSLOT)
        k0 = jnp.maximum(k, 0)

        @pl.when(active)
        def _():
            own_k = rem(k, 8) == me

            hand = hands_on(k)
            for h in (0, 1):
                @pl.when(jnp.logical_and(k >= 2 - h, jnp.logical_not(own_k)))
                def _():
                    ls_copy(3, k, h).wait_recv()

                    @pl.when(hand)
                    def _():
                        ls_copy(3, k, h).start()

            aslot = rem(k, NA)
            ls0 = split3(ls_ref[rem(k, NP), 0])
            ls1 = split3(ls_ref[rem(k, NP), 1])
            lane0 = pl.multiple_of(rem(k, 2) * NB, NB)

            def update(ph):
                n = 1024 - NB * ph
                rows = pl.ds(NB * ph, n)

                @pl.when(rem(k, 2) == c)
                def _():
                    s_ref[rows, :] = ac_ref[aslot, ph:8].reshape(n, NB)

                @pl.when(rem(k, 2) != c)
                def _():
                    for i in range(ph, 8):
                        s_ref[i * NB:(i + 1) * NB, :] = ac_ref[aslot, i].T

                acc = dot6(lh_ref[slot_1, rows, :], ls1) + dot6(lh_ref[slot_2, rows, :], ls0)
                s_ref[rows, :] = s_ref[rows, :] - (u_ref[div(k, 2), rows, pl.ds(lane0, NB)] + acc)
            phases(k + 1, me, update)

            @pl.when(jnp.logical_and(r != rem(k, 2), k + NA < NBLK))
            def _():
                pl.semaphore_signal(a_free, inc=1, device_id=dev(SIB), device_id_type=MESH)

            @pl.when(jnp.logical_and(nxt < NBLK, rem(nxt, 8) == me))
            def _():
                i_n = div(nxt, 8)
                lane_n = pl.multiple_of(rem(nxt, 2) * NB, NB)
                rows_n = pl.ds(pl.multiple_of(i_n * NB, NB), NB)
                p1 = g_ref[slot_1, me, i_n]
                p2 = g_ref[slot_2, me, i_n]
                d_ref[...] = (ac_ref[rem(nxt, NA), i_n] - u_ref[div(nxt, 2), rows_n, pl.ds(lane_n, NB)]
                              - (dot_nt(p1, p1) + dot_nt(p2, p2)))

            @pl.when(jnp.logical_not(own_k))
            def _():
                li_copy(3, k).wait_recv()

                @pl.when(hand)
                def _():
                    li_copy(3, k).start()

        @pl.when(jnp.logical_and(nxt < NBLK, rem(nxt, 8) == me))
        def _():
            i_n = div(nxt, 8)
            sl = rem(nxt, NP)
            rows_n = pl.ds(pl.multiple_of(i_n * NB, NB), NB)

            @pl.when(k < 0)
            def _():
                d_ref[...] = ac_ref[0, 0]

            @pl.when(k >= 0)
            def _():
                xs = dot_nt(s_ref[rows_n, :], li_ref[rem(k0, NP)])
                ls_ref[sl, 1] = xs
                for n in range(4):
                    ls_copy(n, nxt, 1).start()
                d_ref[...] = d_ref[...] - dot_nt(xs, xs)

            cholinv(d_ref, li_ref.at[sl], lt_ref)
            for n in range(4):
                li_copy(n, nxt).start()
            ri = lax.broadcasted_iota(jnp.int32, (NB, NB), 0)
            ci = lax.broadcasted_iota(jnp.int32, (NB, NB), 1)
            lkk_ref[sl] = jnp.where(ri >= ci, lt_ref[...].T, 0.0)
            lk_copy(1, nxt).start()

            @pl.when(r != c)
            def _():
                lk_copy(0, nxt).start()

        @pl.when(active)
        def _():
            li = li_ref[rem(k, NP)]

            li3 = split3(li)

            def solve(ph):
                n = 1024 - NB * ph
                rows = pl.ds(NB * ph, n)
                x = dot6(parts_lhs(s_ref[rows, :]), li3)
                g_ref[slot_k, me, ph:8] = x.reshape(8 - ph, NB, NB)
                lh_ref[slot_k, rows, :] = parts_lhs(x)
            phases(k + 1, me, solve)

            @pl.when(jnp.logical_and(k + 2 < NBLK, rem(k + 2, 8) == me))
            def _():
                ls_ref[rem(k + 2, NP), 0] = g_ref[slot_k, me, div(k + 2, 8)]
                for n in range(4):
                    ls_copy(n, k + 2, 0).start()

            @pl.when(rem(k, 8) == me)
            def _():
                lk_copy(1, k).wait_send()

                @pl.when(r != c)
                def _():
                    lk_copy(0, k).wait_send()
            for n in range(4):
                sent = rem(k, 8) == me
                if n == 3:
                    sent = jnp.logical_or(sent, hands_on(k))

                @pl.when(sent)
                def _():
                    li_copy(n, k).wait_send()
                for h in (0, 1):
                    @pl.when(jnp.logical_and(sent, k >= 2 - h))
                    def _():
                        ls_copy(n, k, h).wait_send()

            @pl.when(k >= NSLOT)
            def _():
                for t in range(3):
                    pl.semaphore_wait(credit.at[t], 1)

            def send(ph):
                for t in range(3):
                    piece_copy(t, slot_k, me, ph, False).start()
            phases(k + 3, me, send)

            @pl.when(jnp.logical_and(jnp.logical_and(r == c, rem(k, 2) == c), rem(k, 8) != me))
            def _():
                lk_copy(0, k).wait_recv()
            row_outs(k, lambda n: row_copy(n, k).start())

        @pl.when(jnp.logical_and(k >= 1, k <= NBLK))
        def _():
            for t in (1, 2):
                cls = class_of(*partner(groups[t]))

                def fwd(ph):
                    piece_copy(t, slot_1, cls, ph, False).wait_recv()
                    piece_copy(t, slot_1, cls, ph, True).start()
                    relay(k - 1, slot_1, cls, ph, t, lambda cp: cp.start())
                phases(k + 2, cls, fwd)

        @pl.when(k >= 2)
        def _():
            m = k - 2
            dg_cls = class_of(*partner(DG))

            def fwd_dg(ph):
                for t in (1, 2):
                    relay(m, slot_2, dg_cls, ph, t, lambda cp: cp.wait_recv())
                piece_copy(3, slot_2, dg_cls, ph, True).start()
            phases(m + 3, dg_cls, fwd_dg)

            sib_cls = class_of(*partner(SIB))
            phases(m + 3, sib_cls, lambda ph: piece_copy(0, slot_2, sib_cls, ph, False).wait_recv())
            for t in range(1, 4):
                cls = class_of(*partner(xor_sib(groups[t])))
                phases(m + 3, cls, lambda ph: piece_copy(t, slot_2, cls, ph, True).wait_recv())

            @pl.when(rem(m, 2) == c)
            def _():
                for e in range(4):
                    phases(m + 3, 2 * e + r, lambda ph: out_copy(m, ph, e).start())

            start = div(m + 3, 2)
            for v in range(8):
                rows = pl.ds(NB * v, 1024 - NB * v)

                def bulk(jp, v=v, rows=rows):
                    jc = 2 * rem(jp, 4)
                    w0 = split3(g_ref[slot_2, jc, v])
                    w1 = split3(g_ref[slot_2, jc + 1, v])
                    w = [jnp.concatenate([x0, x1], axis=0) for x0, x1 in zip(w0, w1)]
                    u_ref[jp, rows, :] = u_ref[jp, rows, :] + dot6(lh_ref[slot_2, rows, :], w)

                @pl.when(start <= 4 * v)
                def _():
                    for q in range(4):
                        bulk(4 * v + q)

                @pl.when(jnp.logical_and(start > 4 * v, start < 4 * v + 4))
                def _():
                    def one(jp, _):
                        bulk(jp)
                        return 0
                    lax.fori_loop(start, 4 * v + 4, one, 0)

            def finish(ph):
                for t in range(3):
                    piece_copy(t, slot_2, me, ph, False).wait_send()
            phases(m + 3, me, finish)
            for t in range(1, 4):
                cls = class_of(*partner(groups[t]))

                def finish_fwd(ph):
                    piece_copy(t, slot_2, cls, ph, True).wait_send()
                    if t < 3:
                        relay(m, slot_2, cls, ph, t, lambda cp: cp.wait_send())
                phases(m + 3, cls, finish_fwd)

            @pl.when(rem(m, 2) == c)
            def _():
                for e in range(4):
                    phases(m + 3, 2 * e + r, lambda ph: out_copy(m, ph, e).wait())

            @pl.when(m + NSLOT < NBLK)
            def _():
                for t in range(3):
                    pl.semaphore_signal(credit.at[t], inc=1, device_id=dev(groups[t]), device_id_type=MESH)

        @pl.when(active)
        def _():
            row_outs(k, lambda n: row_copy(n, k).wait())

        @pl.when(k + 4 < NBLK)
        def _():
            @pl.when(jnp.logical_and(k >= 2, rem(k0, 2) == r))
            def _():
                pl.semaphore_wait(a_free, 1)
            fetch(k + 4)
        return 0

    lax.fori_loop(0, NBLK + 3, step, 0)


def solution(mesh):
    grid_spec = P(("b", "row"), "col")

    def local_factor(a_loc):
        a6 = a_loc.reshape(8, 4, 8, 4, NB, NB)
        dma = pltpu.SemaphoreType.DMA
        fac = pl.pallas_call(
            kernel,
            out_shape=jax.ShapeDtypeStruct((8, 4, 8, 4, NB, NB), F32),
            in_specs=[pl.BlockSpec(memory_space=pl.ANY)],
            out_specs=pl.BlockSpec(memory_space=pl.ANY),
            scratch_shapes=[
                pltpu.VMEM((32, 1024, 256), F32),
                pltpu.VMEM((NSLOT, 8, 8, NB, NB), F32),
                pltpu.VMEM((NA, 8, NB, NB), F32),
                pltpu.VMEM((1024, NB), F32),
                pltpu.VMEM((NP, 2, NB, NB), F32),
                pltpu.VMEM((NP, NB, NB), F32),
                pltpu.VMEM((NP, NB, NB), F32),
                pltpu.VMEM((NB, NB), F32),
                pltpu.VMEM((NB, NB), F32),
                pltpu.VMEM((NSLOT, 1024, 384), BF16),
                dma((3, 4)),
                dma((NP,)),
                dma((NP, 2)),
                dma((NSLOT, 8)),
                dma((NSLOT, 8)),
                pltpu.SemaphoreType.REGULAR((3,)),
                dma((NA,)),
                dma((NA,)),
                dma((NA,)),
                dma((4,)),
                dma((3,)),
                dma((2,)),
                dma((NP,)),
                pltpu.SemaphoreType.REGULAR,
            ],
            compiler_params=pltpu.CompilerParams(
                collective_id=0, has_side_effects=True, vmem_limit_bytes=67043328),
            name="chol_all",
        )(a6)
        fac = fac.reshape(32, 32, NB, NB)
        gi = 2 * jnp.arange(32) + lax.axis_index("row")
        gj = 2 * jnp.arange(32) + lax.axis_index("col")
        keep = gi[:, None] >= gj[None, :]
        return jnp.where(keep[:, :, None, None], fac, 0.0)

    return jax.shard_map(local_factor, mesh=mesh, in_specs=grid_spec, out_specs=grid_spec, check_vma=False)
```

```python
import jax
import jax.numpy as jnp
from jax import lax
from jax.experimental import pallas as pl
from jax.experimental.pallas import tpu as pltpu
from jax.sharding import PartitionSpec as P

MESH = pl.DeviceIdType.MESH
F32 = jnp.float32
BF16 = jnp.bfloat16
NBLK = 64
NB = 128
NSLOT = 4
NA = 6
NP = 16


def bc(x):
    return jnp.broadcast_to(x, (8, 128))

def cholinv(r_ref, z_ref, lt_ref):
    G = 16
    rowi = lax.broadcasted_iota(jnp.int32, (8, 128), 0)
    lanei = lax.broadcasted_iota(jnp.int32, (8, 128), 1)
    for g in range(G):
        z_ref[8*g:8*g+8, :] = jnp.where(lanei == rowi + 8*g, 1.0, 0.0).astype(F32)
    for g in range(G):
        rg = r_ref[8*g:8*g+8, :]
        zg = z_ref[8*g:8*g+8, :]
        c = [bc(rg[:, 8*g+j:8*g+j+1]) for j in range(8)]
        m = [[bc(c[b][a:a+1, :]) for b in range(a+1)] for a in range(8)]
        rr = [None]*8
        l = [[None]*8 for _ in range(8)]
        x = [[None]*8 for _ in range(8)]
        for j in range(8):
            rr[j] = lax.rsqrt(m[j][j])
            for a in range(j+1, 8):
                l[a][j] = m[a][j]*rr[j]
            for a in range(j+1, 8):
                for b in range(j+1, a+1):
                    m[a][b] = m[a][b] - l[a][j]*l[b][j]
            x[j][j] = rr[j]
            for b in range(j):
                s = l[j][b]*x[b][b]
                for cc in range(b+1, j):
                    s = s + l[j][cc]*x[cc][b]
                x[j][b] = -(rr[j]*s)
        rb = [bc(rg[j:j+1, :]) for j in range(8)]
        zb = [bc(zg[j:j+1, :]) for j in range(8)]

        def app(vb):
            y = []
            for i in range(8):
                s = vb[i]
                for j in range(i):
                    s = s - l[i][j]*y[j]
                y.append(s*rr[i])
            w = []
            for j in range(8):
                s = x[j][j]*y[j]
                for i in range(j+1, 8):
                    s = s + x[i][j]*y[i]
                w.append(s)
            return y, w
        y, w = app(rb)
        yz, wz = app(zb)
        yp, zp = y[0], yz[0]
        for i in range(1, 8):
            yp = jnp.where(rowi == i, y[i], yp)
            zp = jnp.where(rowi == i, yz[i], zp)
        lt_ref[8*g:8*g+8, :] = yp
        z_ref[8*g:8*g+8, :] = zp
        for r in range(g+1, min(G, g+1+2)):
            R = r_ref[8*r:8*r+8, :]
            cr = [bc(R[:, 8*g+j:8*g+j+1]) for j in range(8)]
            t = [cr[j]*w[j] for j in range(8)]
            tz = [cr[j]*wz[j] for j in range(8)]
            while len(t) > 1:
                t = [t[i]+t[i+1] for i in range(0, len(t), 2)]
                tz = [tz[i]+tz[i+1] for i in range(0, len(tz), 2)]
            r_ref[8*r:8*r+8, :] = R - t[0]
            z_ref[8*r:8*r+8, :] = z_ref[8*r:8*r+8, :] - tz[0]
        if g + 1 + 2 < G:
            r0 = 8*(g+1+2)
            s1, s2, s3 = split3(jnp.concatenate([yp, zp], axis=1))
            rhs = jnp.concatenate([s1, s2, s1, s2, s3, s1], axis=0)
            a1, a2, a3 = split3(yp)
            lhs = jnp.concatenate([a1, a1, a2, a2, a1, a3], axis=0)
            far = lax.dot_general(lhs, rhs, (((0,), (0,)), ((), ())), preferred_element_type=F32)
            r_ref[r0:128, :] = r_ref[r0:128, :] - far[r0:128, 0:128]
            z_ref[r0:128, :] = z_ref[r0:128, :] - far[r0:128, 128:256]


def dot_bf(a, b):
    return lax.dot_general(a, b, (((1,), (1,)), ((), ())), preferred_element_type=F32)


def split3(w):
    b1 = w.astype(BF16)
    r1 = w - b1.astype(F32)
    b2 = r1.astype(BF16)
    r2 = r1 - b2.astype(F32)
    return b1, b2, r2.astype(BF16)


def dot6(lhs, rhs):
    b1, b2, b3 = rhs
    acc = dot_bf(lhs[:, 0:256], jnp.concatenate([b1, b1], axis=1))
    acc = acc + dot_bf(lhs[:, 0:256], jnp.concatenate([b2, b2], axis=1))
    return acc + dot_bf(lhs[:, 128:384], jnp.concatenate([b3, b1], axis=1))


def parts_lhs(x):
    b1, b2, b3 = split3(x)
    return jnp.concatenate([b2, b1, b3], axis=1)


def kernel(a_ref, out_ref, u_ref, g_ref, ac_ref, s_ref, ls_ref, li_ref, lkk_ref, d_ref, lt_ref, lh_ref,
           pri_send, li_recv, ls_recv, g_send, g_recv, credit, a_loc, a_send, a_recv, o_sem,
           o3_sem, lk_send, lk_recv, a_free):
    div, rem = lax.div, lax.rem
    p, c, r = lax.axis_index("rep"), lax.axis_index("col"), lax.axis_index("row")

    def class_of(pp, cc, rr):
        return cc + 2 * (2 * pp + rem(pp + rr, 2))

    me = class_of(p, c, r)
    flips = [(0, 1, 0), (0, 1, 1), (0, 0, 1), (1, 1, 0), (1, 1, 1), (1, 0, 0), (1, 0, 1)]

    def partner(fl):
        pp = 1 - p if fl[0] else p
        cc = 1 - c if fl[1] else c
        rr = 1 - r if fl[2] else r
        return pp, cc, rr

    def dev(fl):
        pp, cc, rr = partner(fl)
        return {"rep": pp, "col": cc, "row": rr}

    SIB, XN, YN, DG = (0, 0, 1), (0, 1, 0), (1, 0, 0), (1, 1, 0)
    groups = [SIB, XN, YN, DG]

    def xor_sib(fl):
        return (fl[0], fl[1], 1 - fl[2])

    my_q = div(me, 2)
    sib_q = div(class_of(p, c, 1 - r), 2)

    def fetch_src(col, q):
        kk = div(col, 2)
        jj, qq = div(kk, 4), rem(kk, 4)
        nat = a_ref.at[:, q, jj, qq]
        tra = a_ref.at[jj, qq, :, q]
        return nat, tra

    def fetch(col):
        slot = rem(col, NA)

        @pl.when(rem(col, 2) == r)
        def _():
            nat0, tra0 = fetch_src(col, my_q)
            nat1, tra1 = fetch_src(col, sib_q)

            @pl.when(r == c)
            def _():
                pltpu.make_async_copy(nat0, ac_ref.at[slot], a_loc.at[slot]).start()
                pltpu.make_async_remote_copy(nat1, ac_ref.at[slot], a_send.at[slot], a_recv.at[slot],
                                             device_id=dev(SIB), device_id_type=MESH).start()

            @pl.when(r != c)
            def _():
                pltpu.make_async_copy(tra0, ac_ref.at[slot], a_loc.at[slot]).start()
                pltpu.make_async_remote_copy(tra1, ac_ref.at[slot], a_send.at[slot], a_recv.at[slot],
                                             device_id=dev(SIB), device_id_type=MESH).start()

    def fetch_wait(col):
        slot = rem(col, NA)
        cp = pltpu.make_async_remote_copy(ac_ref.at[slot], ac_ref.at[slot], a_send.at[slot], a_recv.at[slot],
                                          device_id=dev(SIB), device_id_type=MESH)

        @pl.when(rem(col, 2) == r)
        def _():
            pltpu.make_async_copy(ac_ref.at[slot], ac_ref.at[slot], a_loc.at[slot]).wait()
            cp.wait_send()

        @pl.when(rem(col, 2) != r)
        def _():
            cp.wait_recv()

    zb = jnp.zeros((NB, NB), F32)
    for s in range(2):
        for h in range(2):
            ls_ref[s, h] = zb
    barrier = pltpu.get_barrier_semaphore()
    for fl in flips:
        pl.semaphore_signal(barrier, inc=1, device_id=dev(fl), device_id_type=MESH)
    pl.semaphore_wait(barrier, 7)
    for col in range(3):
        fetch(jnp.int32(col))

    def zero_u(t, _):
        u_ref[t] = jnp.zeros((1024, 256), F32)
        return 0

    lax.fori_loop(0, 32, zero_u, 0)
    for s in (2, 3):
        lh_ref[s] = jnp.zeros((1024, 384), BF16)
        for i in range(8):
            g_ref[s, me, i] = zb

    def pri_dev(n, k):
        if n == 3:
            return dev(SIB)
        pp, cc, _ = partner([XN, DG, YN][n])
        rr = jnp.where(rem(k, 4) == 1, 1 - r, r)
        return {"rep": pp, "col": cc, "row": rr}

    def li_copy(n, k):
        slot = rem(k, NP)
        return pltpu.make_async_remote_copy(li_ref.at[slot], li_ref.at[slot], pri_send.at[0, n], li_recv.at[slot],
                                            device_id=pri_dev(n, k), device_id_type=MESH)

    def ls_copy(n, k, h):
        slot = rem(k, NP)
        return pltpu.make_async_remote_copy(ls_ref.at[slot, h], ls_ref.at[slot, h], pri_send.at[1 + h, n],
                                            ls_recv.at[slot, h], device_id=pri_dev(n, k), device_id_type=MESH)

    def lk_copy(n, k):
        slot = rem(k, NP)
        to = {"rep": p if n == 0 else 1 - p, "col": c, "row": c}
        return pltpu.make_async_remote_copy(lkk_ref.at[slot], lkk_ref.at[slot], lk_send.at[n], lk_recv.at[slot],
                                            device_id=to, device_id_type=MESH)

    def row_copy(n, k):
        src = [ls_ref.at[rem(k, NP), 0], ls_ref.at[rem(k, NP), 1], lkk_ref.at[rem(k, NP)]][n]
        kk = div(k - [2, 1, 0][n], 2)
        return pltpu.make_async_copy(src, out_ref.at[div(k, 8), div(rem(k, 8), 2), div(kk, 4), rem(kk, 4)], o3_sem.at[n])

    def row_outs(k, fn):
        @pl.when(jnp.logical_and(rem(k, 2) == r, c != r))
        def _():
            @pl.when(k >= 1)
            def _():
                fn(1)

        @pl.when(jnp.logical_and(rem(k, 2) == r, c == r))
        def _():
            fn(2)

            @pl.when(k >= 2)
            def _():
                fn(0)

    def hands_on(k):
        q_o = rem(div(k, 2), 4)
        p_o = div(q_o, 2)
        r_o = rem(q_o + p_o, 2)
        turn = jnp.where(rem(k, 4) == 1, 1, 0)
        away = jnp.logical_or(p != p_o, c != rem(k, 2))
        return jnp.logical_and(away, r == rem(r_o + turn, 2))

    def piece_copy(t, slot, cls, ph, via):
        src = g_ref.at[slot, cls, pl.ds(ph, 8 - ph)]
        to = SIB if via else groups[t]
        idx = 3 + t if via else t
        return pltpu.make_async_remote_copy(src, src, g_send.at[slot, idx], g_recv.at[slot, idx],
                                            device_id=dev(to), device_id_type=MESH)

    def relay_copy(slot, cls, ph, h, t):
        lo, hi = (ph, ph + h) if t == 1 else (ph + h, 8)
        src = g_ref.at[slot, cls, pl.ds(lo, hi - lo)]
        idx = 3 if t == 1 else 7
        return pltpu.make_async_remote_copy(src, src, g_send.at[slot, idx], g_recv.at[slot, idx],
                                            device_id=dev(YN if t == 1 else XN), device_id_type=MESH)

    def relay(k, slot, cls, ph, t, fn):
        n = 8 - ph
        if n % 2 == 0:
            fn(relay_copy(slot, cls, ph, n // 2, t))
        else:
            for par in (0, 1):
                h = (n + par) // 2
                if (h if t == 1 else n - h) > 0:
                    @pl.when(rem(k, 2) == par)
                    def _():
                        fn(relay_copy(slot, cls, ph, h, t))

    def first_of(k, cls):
        return div(k - cls + 7, 8)

    def phases(k, cls, fn):
        for ph in range(8):
            @pl.when(first_of(k, cls) == ph)
            def _():
                fn(ph)

    def out_copy(m, ph, e):
        kk = div(m, 2)
        return pltpu.make_async_copy(g_ref.at[rem(m, NSLOT), 2 * e + r, pl.ds(ph, 8 - ph)],
                                     out_ref.at[pl.ds(ph, 8 - ph), e, div(kk, 4), rem(kk, 4)], o_sem.at[e])

    def step(kp1, _):
        k = kp1 - 1
        nxt = kp1

        @pl.when(nxt < NBLK)
        def _():
            fetch_wait(nxt)

        active = jnp.logical_and(k >= 0, k < NBLK)
        slot_k = rem(k + 4, NSLOT)
        slot_1 = rem(k + 3, NSLOT)
        slot_2 = rem(k + 2, NSLOT)
        k0 = jnp.maximum(k, 0)

        @pl.when(active)
        def _():
            own_k = rem(k, 8) == me

            hand = hands_on(k)
            for h in (0, 1):
                @pl.when(jnp.logical_and(k >= 2 - h, jnp.logical_not(own_k)))
                def _():
                    ls_copy(3, k, h).wait_recv()

                    @pl.when(hand)
                    def _():
                        ls_copy(3, k, h).start()

            aslot = rem(k, NA)
            ls0 = split3(ls_ref[rem(k, NP), 0])
            ls1 = split3(ls_ref[rem(k, NP), 1])
            lane0 = pl.multiple_of(rem(k, 2) * NB, NB)

            def update(ph):
                n = 1024 - NB * ph
                rows = pl.ds(NB * ph, n)

                @pl.when(rem(k, 2) == c)
                def _():
                    s_ref[rows, :] = ac_ref[aslot, ph:8].reshape(n, NB)

                @pl.when(rem(k, 2) != c)
                def _():
                    for i in range(ph, 8):
                        s_ref[i * NB:(i + 1) * NB, :] = ac_ref[aslot, i].T

                acc = dot6(lh_ref[slot_1, rows, :], ls1) + dot6(lh_ref[slot_2, rows, :], ls0)
                s_ref[rows, :] = s_ref[rows, :] - (u_ref[div(k, 2), rows, pl.ds(lane0, NB)] + acc)
            phases(k + 1, me, update)

            @pl.when(jnp.logical_and(r != rem(k, 2), k + NA < NBLK))
            def _():
                pl.semaphore_signal(a_free, inc=1, device_id=dev(SIB), device_id_type=MESH)

            @pl.when(jnp.logical_and(nxt < NBLK, rem(nxt, 8) == me))
            def _():
                i_n = div(nxt, 8)
                lane_n = pl.multiple_of(rem(nxt, 2) * NB, NB)
                rows_n = pl.ds(pl.multiple_of(i_n * NB, NB), NB)
                p1 = g_ref[slot_1, me, i_n]
                p2 = g_ref[slot_2, me, i_n]
                d_ref[...] = (ac_ref[rem(nxt, NA), i_n] - u_ref[div(nxt, 2), rows_n, pl.ds(lane_n, NB)]
                              - (dot6(parts_lhs(p1), split3(p1)) + dot6(parts_lhs(p2), split3(p2))))

            @pl.when(jnp.logical_not(own_k))
            def _():
                li_copy(3, k).wait_recv()

                @pl.when(hand)
                def _():
                    li_copy(3, k).start()

        @pl.when(jnp.logical_and(nxt < NBLK, rem(nxt, 8) == me))
        def _():
            i_n = div(nxt, 8)
            sl = rem(nxt, NP)
            rows_n = pl.ds(pl.multiple_of(i_n * NB, NB), NB)

            @pl.when(k < 0)
            def _():
                d_ref[...] = ac_ref[0, 0]

            @pl.when(k >= 0)
            def _():
                xs = dot6(parts_lhs(s_ref[rows_n, :]), split3(li_ref[rem(k0, NP)]))
                ls_ref[sl, 1] = xs
                for n in range(4):
                    ls_copy(n, nxt, 1).start()
                d_ref[...] = d_ref[...] - dot6(parts_lhs(xs), split3(xs))

            cholinv(d_ref, li_ref.at[sl], lt_ref)
            for n in range(4):
                li_copy(n, nxt).start()
            ri = lax.broadcasted_iota(jnp.int32, (NB, NB), 0)
            ci = lax.broadcasted_iota(jnp.int32, (NB, NB), 1)
            lkk_ref[sl] = jnp.where(ri >= ci, lt_ref[...].T, 0.0)
            lk_copy(1, nxt).start()

            @pl.when(r != c)
            def _():
                lk_copy(0, nxt).start()

        @pl.when(active)
        def _():
            li = li_ref[rem(k, NP)]

            li3 = split3(li)

            def solve(ph):
                n = 1024 - NB * ph
                rows = pl.ds(NB * ph, n)
                x = dot6(parts_lhs(s_ref[rows, :]), li3)
                g_ref[slot_k, me, ph:8] = x.reshape(8 - ph, NB, NB)
                lh_ref[slot_k, rows, :] = parts_lhs(x)
            phases(k + 1, me, solve)

            @pl.when(jnp.logical_and(k + 2 < NBLK, rem(k + 2, 8) == me))
            def _():
                ls_ref[rem(k + 2, NP), 0] = g_ref[slot_k, me, div(k + 2, 8)]
                for n in range(4):
                    ls_copy(n, k + 2, 0).start()

            @pl.when(rem(k, 8) == me)
            def _():
                lk_copy(1, k).wait_send()

                @pl.when(r != c)
                def _():
                    lk_copy(0, k).wait_send()
            for n in range(4):
                sent = rem(k, 8) == me
                if n == 3:
                    sent = jnp.logical_or(sent, hands_on(k))

                @pl.when(sent)
                def _():
                    li_copy(n, k).wait_send()
                for h in (0, 1):
                    @pl.when(jnp.logical_and(sent, k >= 2 - h))
                    def _():
                        ls_copy(n, k, h).wait_send()

            @pl.when(k >= NSLOT)
            def _():
                for t in range(3):
                    pl.semaphore_wait(credit.at[t], 1)

            def send(ph):
                for t in range(3):
                    piece_copy(t, slot_k, me, ph, False).start()
            phases(k + 3, me, send)

            @pl.when(jnp.logical_and(jnp.logical_and(r == c, rem(k, 2) == c), rem(k, 8) != me))
            def _():
                lk_copy(0, k).wait_recv()
            row_outs(k, lambda n: row_copy(n, k).start())

        @pl.when(jnp.logical_and(k >= 1, k <= NBLK))
        def _():
            for t in (1, 2):
                cls = class_of(*partner(groups[t]))

                def fwd(ph):
                    piece_copy(t, slot_1, cls, ph, False).wait_recv()
                    piece_copy(t, slot_1, cls, ph, True).start()
                    relay(k - 1, slot_1, cls, ph, t, lambda cp: cp.start())
                phases(k + 2, cls, fwd)

        @pl.when(k >= 2)
        def _():
            m = k - 2
            dg_cls = class_of(*partner(DG))

            def fwd_dg(ph):
                for t in (1, 2):
                    relay(m, slot_2, dg_cls, ph, t, lambda cp: cp.wait_recv())
                piece_copy(3, slot_2, dg_cls, ph, True).start()
            phases(m + 3, dg_cls, fwd_dg)

            sib_cls = class_of(*partner(SIB))
            phases(m + 3, sib_cls, lambda ph: piece_copy(0, slot_2, sib_cls, ph, False).wait_recv())
            for t in range(1, 4):
                cls = class_of(*partner(xor_sib(groups[t])))
                phases(m + 3, cls, lambda ph: piece_copy(t, slot_2, cls, ph, True).wait_recv())

            @pl.when(rem(m, 2) == c)
            def _():
                for e in range(4):
                    phases(m + 3, 2 * e + r, lambda ph: out_copy(m, ph, e).start())

            start = div(m + 3, 2)
            for v in range(8):
                rows = pl.ds(NB * v, 1024 - NB * v)

                def bulk(jp, v=v, rows=rows):
                    jc = 2 * rem(jp, 4)
                    w0 = split3(g_ref[slot_2, jc, v])
                    w1 = split3(g_ref[slot_2, jc + 1, v])
                    w = [jnp.concatenate([x0, x1], axis=0) for x0, x1 in zip(w0, w1)]
                    u_ref[jp, rows, :] = u_ref[jp, rows, :] + dot6(lh_ref[slot_2, rows, :], w)

                @pl.when(start <= 4 * v)
                def _():
                    for q in range(4):
                        bulk(4 * v + q)

                @pl.when(jnp.logical_and(start > 4 * v, start < 4 * v + 4))
                def _():
                    def one(jp, _):
                        bulk(jp)
                        return 0
                    lax.fori_loop(start, 4 * v + 4, one, 0)

            def finish(ph):
                for t in range(3):
                    piece_copy(t, slot_2, me, ph, False).wait_send()
            phases(m + 3, me, finish)
            for t in range(1, 4):
                cls = class_of(*partner(groups[t]))

                def finish_fwd(ph):
                    piece_copy(t, slot_2, cls, ph, True).wait_send()
                    if t < 3:
                        relay(m, slot_2, cls, ph, t, lambda cp: cp.wait_send())
                phases(m + 3, cls, finish_fwd)

            @pl.when(rem(m, 2) == c)
            def _():
                for e in range(4):
                    phases(m + 3, 2 * e + r, lambda ph: out_copy(m, ph, e).wait())

            @pl.when(m + NSLOT < NBLK)
            def _():
                for t in range(3):
                    pl.semaphore_signal(credit.at[t], inc=1, device_id=dev(groups[t]), device_id_type=MESH)

        @pl.when(active)
        def _():
            row_outs(k, lambda n: row_copy(n, k).wait())

        @pl.when(k + 4 < NBLK)
        def _():
            @pl.when(jnp.logical_and(k >= 2, rem(k0, 2) == r))
            def _():
                pl.semaphore_wait(a_free, 1)
            fetch(k + 4)
        return 0

    lax.fori_loop(0, NBLK + 3, step, 0)


def solution(mesh):
    grid_spec = P(("b", "row"), "col")

    def local_factor(a_loc):
        a6 = a_loc.reshape(8, 4, 8, 4, NB, NB)
        dma = pltpu.SemaphoreType.DMA
        fac = pl.pallas_call(
            kernel,
            out_shape=jax.ShapeDtypeStruct((8, 4, 8, 4, NB, NB), F32),
            in_specs=[pl.BlockSpec(memory_space=pl.ANY)],
            out_specs=pl.BlockSpec(memory_space=pl.ANY),
            scratch_shapes=[
                pltpu.VMEM((32, 1024, 256), F32),
                pltpu.VMEM((NSLOT, 8, 8, NB, NB), F32),
                pltpu.VMEM((NA, 8, NB, NB), F32),
                pltpu.VMEM((1024, NB), F32),
                pltpu.VMEM((NP, 2, NB, NB), F32),
                pltpu.VMEM((NP, NB, NB), F32),
                pltpu.VMEM((NP, NB, NB), F32),
                pltpu.VMEM((NB, NB), F32),
                pltpu.VMEM((NB, NB), F32),
                pltpu.VMEM((NSLOT, 1024, 384), BF16),
                dma((3, 4)),
                dma((NP,)),
                dma((NP, 2)),
                dma((NSLOT, 8)),
                dma((NSLOT, 8)),
                pltpu.SemaphoreType.REGULAR((3,)),
                dma((NA,)),
                dma((NA,)),
                dma((NA,)),
                dma((4,)),
                dma((3,)),
                dma((2,)),
                dma((NP,)),
                pltpu.SemaphoreType.REGULAR,
            ],
            compiler_params=pltpu.CompilerParams(
                collective_id=0, has_side_effects=True, vmem_limit_bytes=67043328),
            name="chol_all",
        )(a6)
        fac = fac.reshape(32, 32, NB, NB)
        gi = 2 * jnp.arange(32) + lax.axis_index("row")
        gj = 2 * jnp.arange(32) + lax.axis_index("col")
        keep = gi[:, None] >= gj[None, :]
        return jnp.where(keep[:, :, None, None], fac, 0.0)

    return jax.shard_map(local_factor, mesh=mesh, in_specs=grid_spec, out_specs=grid_spec, check_vma=False)
```
